32 devices in a mesh: blk: 8 (over z, x), rows: 4 (over y, core).
Axes of the slice: x: 2, y: 2, z: 4, core: 2. Of those that a mesh axis runs over, the one named last changes fastest.
Arguments:
- columns: float32 [512, 16384], P('blk', 'rows'), may hold values from -100 to 100
- plan: int32 [3, 16], replicated, may hold values from 0 to 15, as said below
Outputs:
- swept: float32 [512, 16384], P('blk', 'rows')
- off_ratio: float32 [3], replicated
The draws below stay inside these ranges and needn't reach their ends.
Inputs may be any that keep to these rules, and one draw needn't show every extreme that they name: `plan`: row s is a permutation of the 16 positions (position k is slot k % 2 of blk index k // 2). In each row there are a slot t and a number m of 1 to 7 such that the block in slot t of every blk index i goes to slot t of blk index (i + m) modulo 16 / 2, and every other block stays where it is.
All inputs are finite; a program needn't handle non-finite values. Where the reference program divides by a largest or mean magnitude, that divisor is 1e-20 or more.
Results may differ from the reference program's by a relative error of at most 0.00011.
Values sent between devices are 32-bit elements; how exact they have to be, the bound alone decides.
No kernel may reach another device: no remote copies, remote signals or barrier semaphores. Data moves between devices by JAX's collectives and lax.ppermute only.
A program may use at most 64 MiB of HBM per device.

```python
import math
import jax
import jax.numpy as jnp
from jax import lax

BW = 32
STEPS = 3
EIG_ITERS = 3
NS_ITERS = 8
BLOCKS = 16
NCOL = 512
M = 16384


def draw_columns(key, part):
    keys = jax.random.split(jax.random.fold_in(key, 11), 2)
    position = jnp.arange(NCOL, dtype=jnp.float32) / NCOL
    scales = jnp.exp(jax.random.uniform(keys[0], (NCOL,), jnp.float32, 0.0, math.log(6.0)))
    entries = jax.random.normal(keys[1], (NCOL, M), jnp.float32)
    trend = 1.0 + 0.8 * position
    values = entries * (scales * trend)[:, None]
    return jnp.clip(values, -100.0, 100.0).astype(jnp.float32)


def draw_plan(key, part):
    keys = jax.random.split(jax.random.fold_in(key, 23), 2)
    half = BLOCKS // 2
    partner_steps = jax.random.randint(keys[0], (STEPS,), 1, half)
    leaving_slots = jax.random.randint(keys[1], (STEPS,), 0, 2)
    position = jnp.arange(BLOCKS, dtype=jnp.int32)
    device_index = position // 2
    slot_index = position % 2
    moved = (device_index[None, :] + partner_steps[:, None]) % half * 2 + slot_index[None, :]
    table = jnp.where(slot_index[None, :] == leaving_slots[:, None], moved, position[None, :])
    return table.astype(jnp.int32)


def setup_inputs(seed: int = 0) -> dict:
    key_of = jax.random.split(jax.random.key(seed), 3)
    return {
        "columns": draw_columns(jax.random.fold_in(key_of[2], 71), 0),
        "plan": draw_plan(jax.random.fold_in(key_of[2], 71), 0),
    }


PRECISE = lax.Precision.HIGHEST

def matmul(left, right):
    return jnp.matmul(left, right, precision=PRECISE, preferred_element_type=jnp.float32)

def flipped(matrix):
    return jnp.swapaxes(matrix, -1, -2)

def orthonormal(matrix):
    lengths = jnp.sqrt(lax.optimization_barrier(jnp.sum(matrix * matrix, axis=-2, keepdims=True)))
    normed = matrix / lengths
    inner = matmul(flipped(normed), normed)
    bound = lax.optimization_barrier(jnp.max(lax.optimization_barrier(jnp.sum(jnp.abs(inner), axis=-1)), axis=-1))
    normed = normed / jnp.sqrt(bound)[..., None, None]
    for turn_index in range(NS_ITERS):
        normed = 1.5 * normed - 0.5 * matmul(normed, matmul(flipped(normed), normed))
    return normed

def pair_rotation(gram_sum):
    rotation = jnp.broadcast_to(jnp.eye(gram_sum.shape[-1], dtype=gram_sum.dtype), gram_sum.shape)
    for turn_index in range(EIG_ITERS):
        rotation = orthonormal(matmul(gram_sum, rotation))
    return rotation

def reference(columns, plan):
    current = columns
    eye_mask = jnp.eye(2 * BW, dtype=bool)
    ratios = []
    for step_index in range(STEPS):
        pairs = current.reshape(BLOCKS // 2, 2 * BW, M)
        gram_sum = matmul(pairs, flipped(pairs))
        off_part = jnp.where(eye_mask, 0.0, gram_sum)
        diag_part = jnp.where(eye_mask, gram_sum, 0.0)
        off_total = jnp.sum(off_part * off_part)
        diag_total = jnp.sum(diag_part * diag_part)
        ratios.append(jnp.sqrt(off_total) / jnp.sqrt(diag_total))
        rotation = pair_rotation(gram_sum)
        rotated = matmul(flipped(rotation), pairs)
        blocks = rotated.reshape(BLOCKS, BW, M)
        placed = jnp.zeros_like(blocks).at[plan[step_index]].set(blocks)
        current = placed.reshape(NCOL, M)
    return (current, jnp.stack(ratios))
```

```python
from functools import partial

import jax
import jax.numpy as jnp
from jax import lax
from jax.experimental import pallas as pl
from jax.experimental.pallas import tpu as pltpu
from jax.sharding import PartitionSpec as P

STEPS = 3
EIG_ITERS = 3
NS_ITERS = 8
AHEAD = 0.5


def matmul(left, right, contract):
    return lax.dot_general(
        left, right, (contract, ((), ())),
        precision=lax.Precision.HIGH, preferred_element_type=jnp.float32,
    )


def tree_sum(terms):
    terms = list(terms)
    while len(terms) > 1:
        pairs = [terms[i] + terms[i + 1] for i in range(0, len(terms) - 1, 2)]
        if len(terms) % 2:
            pairs.append(terms[-1])
        terms = pairs
    return terms[0]


def exchanged(value, axis, masks):
    count = lax.axis_size(axis)
    got = [value]
    for mask in masks:
        got.append(lax.ppermute(value, axis, [(i, i ^ mask) for i in range(count)]))
    return got


def power_of_two(count):
    return count & (count - 1) == 0


def sum_over_blk(value):
    count = lax.axis_size("blk")
    if not power_of_two(count):
        return lax.psum(value, "blk")
    low = min(count, 4)
    value = tree_sum(exchanged(value, "blk", range(1, low)))
    return tree_sum(exchanged(value, "blk", range(low, count, low)))


def split3(value):
    first = value.astype(jnp.bfloat16)
    rest = value - first.astype(jnp.float32)
    second = rest.astype(jnp.bfloat16)
    third = (rest - second.astype(jnp.float32)).astype(jnp.bfloat16)
    return first, second, third


def dot(left, right):
    return jnp.dot(left, right, preferred_element_type=jnp.float32)


def split_dot(left, right):
    l1, l2, l3 = split3(left)
    r1, r2, r3 = right
    small = dot(l1, r3) + dot(l2, r2) + dot(l3, r1)
    return (small + (dot(l1, r2) + dot(l2, r1))) + dot(l1, r1)


def rotation_kernel(*refs):
    *gram_refs, rotation_ref, sums_ref = refs
    gram = tree_sum([ref[...] for ref in gram_refs])
    size = gram.shape[0]
    row = lax.broadcasted_iota(jnp.int32, gram.shape, 0)
    col = lax.broadcasted_iota(jnp.int32, gram.shape, 1)
    diagonal = row == col
    squares = gram * gram
    off = jnp.sum(jnp.where(diagonal, 0.0, squares))
    diag = jnp.sum(jnp.where(diagonal, squares, 0.0))
    lane = lax.broadcasted_iota(jnp.int32, sums_ref.shape, 1)
    sums_ref[...] = jnp.where(lane == 0, off, jnp.where(lane == 1, diag, 0.0))

    eye15 = jnp.where(diagonal, 1.5, 0.0)
    image = gram
    for turn in range(EIG_ITERS):
        last = turn == EIG_ITERS - 1
        image_parts = split3(image)
        inner = split_dot(image.T if turn else image, image_parts)
        held = image if last else split_dot(gram, image_parts)
        kept = jnp.where(diagonal, inner, 0.0)
        by_col = lax.rsqrt(jnp.sum(kept, axis=0, keepdims=True))
        by_row = lax.rsqrt(jnp.sum(kept, axis=1, keepdims=True))
        inner = (inner * by_row) * by_col
        bound = jnp.max(jnp.sum(jnp.abs(inner), axis=1, keepdims=True), axis=0, keepdims=True)
        inner = inner / bound
        held = (held * by_col) * lax.rsqrt(bound)

        def turn_body(index, carry):
            inner, held = carry
            step = split3(eye15 - 0.5 * inner)
            both = split_dot(jnp.concatenate([inner, held], axis=0), step)
            return split_dot(both[:size], step), both[size:]

        inner, held = lax.fori_loop(0, NS_ITERS - 1, turn_body, (inner, held))
        image = split_dot(held, split3(eye15 - 0.5 * inner))
    rotation_ref[...] = image


def pair_rotation(grams):
    size = grams[0].shape[0]
    return pl.pallas_call(
        rotation_kernel,
        out_shape=(
            jax.ShapeDtypeStruct((size, size), jnp.float32),
            jax.ShapeDtypeStruct((8, 128), jnp.float32),
        ),
        name="pair_rotation",
    )(*grams)


def summed_grams(partial_gram):
    rows = lax.axis_size("rows")
    if not power_of_two(rows):
        return [lax.psum(partial_gram, "rows")]
    return exchanged(partial_gram, "rows", range(1, rows))


def one_step(stay, moved, second_leaves, distance):
    width, length = stay.shape
    ahead = int(length * AHEAD) // 128 * 128
    count = lax.axis_size("blk")
    pairs = [(i, (i + distance) % count) for i in range(count)]

    current = jnp.concatenate([stay, moved], axis=0)
    raw_in = lax.ppermute(current[:, :ahead], "blk", pairs)
    partial_gram = matmul(current, current, ((1,), (1,)))
    rotation, step_sums = pair_rotation(summed_grams(partial_gram))
    leaving = jnp.where(second_leaves, rotation[:, width:], rotation[:, :width])
    staying = jnp.where(second_leaves, rotation[:, :width], rotation[:, width:])
    rest = matmul(leaving, current[:, ahead:], ((0,), (0,)))
    rest_in = lax.ppermute(rest, "blk", pairs)
    leaving_in = lax.ppermute(leaving, "blk", pairs)
    stay = matmul(staying, current, ((0,), (0,)))
    front_in = matmul(leaving_in, raw_in, ((0,), (0,)))
    return stay, jnp.concatenate([front_in, rest_in], axis=1), step_sums[:1]


def local(columns, plan):
    cycle_size = lax.axis_size("blk")
    width = columns.shape[0] // 2
    branches = [partial(one_step, distance=distance) for distance in range(1, cycle_size)]

    def step_body(step_index, carry):
        stay, moved, held_slot, sums = carry
        first_dest = plan[step_index, 0]
        second_dest = plan[step_index, 1]
        partner_step = jnp.maximum(first_dest // 2, second_dest // 2)
        slot = (second_dest != 1).astype(jnp.int32)
        stay, moved, step_sums = lax.switch(
            partner_step - 1, branches, stay, moved, slot == held_slot
        )
        return stay, moved, slot, lax.dynamic_update_slice(sums, step_sums, (step_index, 0))

    carry = (columns[:width], columns[width:], jnp.int32(1), jnp.zeros((STEPS, 128), jnp.float32))
    stay, moved, held_slot, sums = lax.fori_loop(0, STEPS, step_body, carry)
    totals = sum_over_blk(sums)
    current = jnp.where(
        held_slot == 1,
        jnp.concatenate([stay, moved], axis=0),
        jnp.concatenate([moved, stay], axis=0),
    )
    return (current, jnp.sqrt(totals[:, 0]) / jnp.sqrt(totals[:, 1]))


def solution(mesh):
    return jax.shard_map(
        local,
        mesh=mesh,
        in_specs=(P("blk", "rows"), P()),
        out_specs=(P("blk", "rows"), P()),
        check_vma=False,
    )
```

```python
from functools import partial

import jax
import jax.numpy as jnp
from jax import lax
from jax.experimental import pallas as pl
from jax.experimental.pallas import tpu as pltpu
from jax.sharding import PartitionSpec as P

STEPS = 3
EIG_ITERS = 3
NS_ITERS = 8
AHEAD = 0.5


def matmul(left, right, contract):
    return lax.dot_general(
        left, right, (contract, ((), ())),
        precision=lax.Precision.HIGH, preferred_element_type=jnp.float32,
    )


def tree_sum(terms):
    terms = list(terms)
    while len(terms) > 1:
        pairs = [terms[i] + terms[i + 1] for i in range(0, len(terms) - 1, 2)]
        if len(terms) % 2:
            pairs.append(terms[-1])
        terms = pairs
    return terms[0]


def exchanged(value, axis, masks):
    count = lax.axis_size(axis)
    got = [value]
    for mask in masks:
        got.append(lax.ppermute(value, axis, [(i, i ^ mask) for i in range(count)]))
    return got


def power_of_two(count):
    return count & (count - 1) == 0


def sum_over_blk(value):
    count = lax.axis_size("blk")
    if not power_of_two(count):
        return lax.psum(value, "blk")
    low = min(count, 4)
    value = tree_sum(exchanged(value, "blk", range(1, low)))
    return tree_sum(exchanged(value, "blk", range(low, count, low)))


def parts(value):
    first = value.astype(jnp.bfloat16).astype(jnp.float32)
    rest = value - first
    second = rest.astype(jnp.bfloat16).astype(jnp.float32)
    return first, second, rest - second


def dot(left, right):
    return jnp.dot(left, right, preferred_element_type=jnp.float32)


def left_operand(value):
    first, second, third = parts(value)
    low = lax.broadcasted_iota(jnp.int32, value.shape, 1) < value.shape[1] // 2
    return tuple(
        jnp.where(low, one, other).astype(jnp.bfloat16)
        for one, other in ((first, second), (third, first), (second, first))
    )


def right_operand(value):
    first, second, third = (part.astype(jnp.bfloat16) for part in parts(value))
    return tuple(
        jnp.concatenate(pair, axis=0)
        for pair in ((first, first), (first, second), (second, third))
    )


def product(left, right):
    return (dot(left[2], right[2]) + dot(left[1], right[1])) + dot(left[0], right[0])


def transposed(value):
    return jnp.concatenate([value, value], axis=0).T[: value.shape[0]]


def rotation_kernel(flag_ref, *refs):
    *gram_refs, leaving_ref, staying_ref, sums_ref = refs
    gram = tree_sum([ref[...] for ref in gram_refs])
    size = gram.shape[0]
    gram = jnp.concatenate([gram, gram], axis=1)
    row = lax.broadcasted_iota(jnp.int32, gram.shape, 0)
    col = lax.broadcasted_iota(jnp.int32, gram.shape, 1)
    diagonal = (row == col) | (row + size == col)
    squares = gram * gram
    off = 0.5 * jnp.sum(jnp.where(diagonal, 0.0, squares))
    diag = 0.5 * jnp.sum(jnp.where(diagonal, squares, 0.0))
    lane = lax.broadcasted_iota(jnp.int32, sums_ref.shape, 1)
    sums_ref[...] = jnp.where(lane == 0, off, jnp.where(lane == 1, diag, 0.0))

    eye15 = jnp.where(diagonal, 1.5, 0.0)
    gram_left = left_operand(gram)
    image = gram
    for turn in range(EIG_ITERS):
        last = turn == EIG_ITERS - 1
        image_right = right_operand(image)
        inner = product(left_operand(transposed(image)) if turn else gram_left, image_right)
        held = image if last else product(gram_left, image_right)
        kept = jnp.where(diagonal, inner, 0.0)
        by_col = lax.rsqrt(jnp.sum(kept, axis=0, keepdims=True))
        by_row = lax.rsqrt(0.5 * jnp.sum(kept, axis=1, keepdims=True))
        inner = (inner * by_row) * by_col
        row_sums = 0.5 * jnp.sum(jnp.abs(inner), axis=1, keepdims=True)
        bound = jnp.max(row_sums, axis=0, keepdims=True)
        inner = inner / bound
        held = (held * by_col) * lax.rsqrt(bound)

        def turn_body(index, carry):
            inner, held = carry
            step = right_operand(eye15 - 0.5 * inner)
            half = product(left_operand(inner), step)
            held = product(left_operand(held), step)
            return product(left_operand(half), step), held

        inner, held = lax.fori_loop(0, NS_ITERS - 1, turn_body, (inner, held))
        image = product(left_operand(held), right_operand(eye15 - 0.5 * inner))
    first = image[:, : size // 2]
    second = image[:, size // 2 : size]
    second_leaves = flag_ref[0] == 1
    leaving_ref[...] = jnp.where(second_leaves, second, first)
    staying_ref[...] = jnp.where(second_leaves, first, second)


def pair_rotation(flag, grams):
    size = grams[0].shape[0]
    vmem = pl.BlockSpec(memory_space=pltpu.VMEM)
    half = jax.ShapeDtypeStruct((size, size // 2), jnp.float32)
    return pl.pallas_call(
        rotation_kernel,
        in_specs=[pl.BlockSpec(memory_space=pltpu.SMEM)] + [vmem] * len(grams),
        out_specs=(vmem, vmem, vmem),
        out_shape=(half, half, jax.ShapeDtypeStruct((8, 128), jnp.float32)),
        name="pair_rotation",
    )(flag, *grams)


def summed_grams(partial_gram):
    rows = lax.axis_size("rows")
    if not power_of_two(rows):
        return [lax.psum(partial_gram, "rows")]
    return exchanged(partial_gram, "rows", range(1, rows))


def one_step(stay, moved, flag, distance):
    width, length = stay.shape
    ahead = int(length * AHEAD) // 128 * 128
    count = lax.axis_size("blk")
    pairs = [(i, (i + distance) % count) for i in range(count)]

    current = jnp.concatenate([stay, moved], axis=0)
    raw_in = lax.ppermute(current[:, :ahead], "blk", pairs)
    partial_gram = matmul(current, current, ((1,), (1,)))
    leaving, staying, step_sums = pair_rotation(flag, summed_grams(partial_gram))
    rest = matmul(leaving, current[:, ahead:], ((0,), (0,)))
    rest_in = lax.ppermute(rest, "blk", pairs)
    leaving_in = lax.ppermute(leaving, "blk", pairs)
    stay = matmul(staying, current, ((0,), (0,)))
    front_in = matmul(leaving_in, raw_in, ((0,), (0,)))
    return stay, jnp.concatenate([front_in, rest_in], axis=1), step_sums[:1]


def local(columns, plan):
    cycle_size = lax.axis_size("blk")
    width = columns.shape[0] // 2
    branches = [partial(one_step, distance=distance) for distance in range(1, cycle_size)]

    slots = (plan[:, 1] != 1).astype(jnp.int32)
    held = jnp.concatenate([jnp.ones((1,), jnp.int32), slots[:-1]])
    flags = (slots == held).astype(jnp.int32)
    shifts = jnp.maximum(plan[:, 0] >> 1, plan[:, 1] >> 1) - 1
    slots, flags, shifts = lax.optimization_barrier((slots, flags, shifts))

    def step_body(step_index, carry):
        stay, moved, sums = carry
        flag = lax.dynamic_slice(flags, (step_index,), (1,))
        stay, moved, step_sums = lax.switch(shifts[step_index], branches, stay, moved, flag)
        return stay, moved, lax.dynamic_update_slice(sums, step_sums, (step_index, 0))

    carry = (columns[:width], columns[width:], jnp.zeros((STEPS, 128), jnp.float32))
    stay, moved, sums = lax.fori_loop(0, STEPS, step_body, carry)
    totals = sum_over_blk(sums)
    current = jnp.where(
        slots[STEPS - 1] == 1,
        jnp.concatenate([stay, moved], axis=0),
        jnp.concatenate([moved, stay], axis=0),
    )
    return (current, jnp.sqrt(totals[:, 0]) / jnp.sqrt(totals[:, 1]))


def solution(mesh):
    return jax.shard_map(
        local,
        mesh=mesh,
        in_specs=(P("blk", "rows"), P()),
        out_specs=(P("blk", "rows"), P()),
        check_vma=False,
    )
```

```python
from functools import partial

import jax
import jax.numpy as jnp
from jax import lax
from jax.experimental import pallas as pl
from jax.experimental.pallas import tpu as pltpu
from jax.sharding import PartitionSpec as P

STEPS = 3
EIG_ITERS = 3
NS_ITERS = 8
AHEAD_SHORT = 9 / 16
AHEAD_LONG = 5 / 16


def matmul(left, right, contract):
    return lax.dot_general(
        left, right, (contract, ((), ())),
        precision=lax.Precision.HIGH, preferred_element_type=jnp.float32,
    )


def tree_sum(terms):
    terms = list(terms)
    while len(terms) > 1:
        pairs = [terms[i] + terms[i + 1] for i in range(0, len(terms) - 1, 2)]
        if len(terms) % 2:
            pairs.append(terms[-1])
        terms = pairs
    return terms[0]


def exchanged(value, axis, masks):
    count = lax.axis_size(axis)
    got = [value]
    for mask in masks:
        got.append(lax.ppermute(value, axis, [(i, i ^ mask) for i in range(count)]))
    return got


def power_of_two(count):
    return count & (count - 1) == 0


def sum_over_blk(value):
    count = lax.axis_size("blk")
    if not power_of_two(count):
        return lax.psum(value, "blk")
    low = min(count, 4)
    value = tree_sum(exchanged(value, "blk", range(1, low)))
    return tree_sum(exchanged(value, "blk", range(low, count, low)))


def parts(value):
    first = value.astype(jnp.bfloat16).astype(jnp.float32)
    rest = value - first
    second = rest.astype(jnp.bfloat16).astype(jnp.float32)
    return first, second, rest - second


def dot(left, right):
    return jnp.dot(left, right, preferred_element_type=jnp.float32)


def left_operand(value):
    first, second, third = parts(value)
    low = lax.broadcasted_iota(jnp.int32, value.shape, 1) < value.shape[1] // 2
    return tuple(
        jnp.where(low, one, other).astype(jnp.bfloat16)
        for one, other in ((first, second), (third, first), (second, first))
    )


def right_operand(value):
    first, second, third = (part.astype(jnp.bfloat16) for part in parts(value))
    return tuple(
        jnp.concatenate(pair, axis=0)
        for pair in ((first, first), (first, second), (second, third))
    )


def product(left, right):
    return (dot(left[2], right[2]) + dot(left[1], right[1])) + dot(left[0], right[0])


def transposed(value):
    return jnp.concatenate([value, value], axis=0).T[: value.shape[0]]


def rotation_kernel(code_ref, *refs):
    *gram_refs, leaving_ref, staying_ref, sums_ref = refs
    gram = tree_sum([ref[...] for ref in gram_refs])
    size = gram.shape[0]
    gram = jnp.concatenate([gram, gram], axis=1)
    row = lax.broadcasted_iota(jnp.int32, gram.shape, 0)
    col = lax.broadcasted_iota(jnp.int32, gram.shape, 1)
    diagonal = (row == col) | (row + size == col)
    squares = gram * gram
    off = 0.5 * jnp.sum(jnp.where(diagonal, 0.0, squares))
    diag = 0.5 * jnp.sum(jnp.where(diagonal, squares, 0.0))
    lane = lax.broadcasted_iota(jnp.int32, sums_ref.shape, 1)
    sums_ref[...] = jnp.where(lane == 0, off, jnp.where(lane == 1, diag, 0.0))

    eye15 = jnp.where(diagonal, 1.5, 0.0)
    gram_left = left_operand(gram)
    image = gram
    for turn in range(EIG_ITERS):
        last = turn == EIG_ITERS - 1
        image_right = right_operand(image)
        inner = product(left_operand(transposed(image)) if turn else gram_left, image_right)
        held = image if last else product(gram_left, image_right)
        kept = jnp.where(diagonal, inner, 0.0)
        by_col = lax.rsqrt(jnp.sum(kept, axis=0, keepdims=True))
        by_row = lax.rsqrt(0.5 * jnp.sum(kept, axis=1, keepdims=True))
        inner = (inner * by_row) * by_col
        row_sums = 0.5 * jnp.sum(jnp.abs(inner), axis=1, keepdims=True)
        bound = jnp.max(row_sums, axis=0, keepdims=True)
        inner = inner / bound
        held = (held * by_col) * lax.rsqrt(bound)

        def turn_body(index, carry):
            inner, held = carry
            step = right_operand(eye15 - 0.5 * inner)
            half = product(left_operand(inner), step)
            held = product(left_operand(held), step)
            return product(left_operand(half), step), held

        inner, held = lax.fori_loop(0, NS_ITERS - 1, turn_body, (inner, held))
        image = product(left_operand(held), right_operand(eye15 - 0.5 * inner))
    first = image[:, : size // 2]
    second = image[:, size // 2 : size]
    second_leaves = (code_ref[0] & 1) == 1
    leaving_ref[...] = jnp.where(second_leaves, second, first)
    staying_ref[...] = jnp.where(second_leaves, first, second)


def pair_rotation(code, grams):
    size = grams[0].shape[0]
    vmem = pl.BlockSpec(memory_space=pltpu.VMEM)
    half = jax.ShapeDtypeStruct((size, size // 2), jnp.float32)
    return pl.pallas_call(
        rotation_kernel,
        in_specs=[pl.BlockSpec(memory_space=pltpu.SMEM)] + [vmem] * len(grams),
        out_specs=(vmem, vmem, vmem),
        out_shape=(half, half, jax.ShapeDtypeStruct((8, 128), jnp.float32)),
        name="pair_rotation",
    )(code, *grams)


def summed_grams(partial_gram):
    rows = lax.axis_size("rows")
    if not power_of_two(rows):
        return [lax.psum(partial_gram, "rows")]
    return exchanged(partial_gram, "rows", range(1, rows))


def one_step(stay, moved, code, distance):
    width, length = stay.shape
    count = lax.axis_size("blk")
    long_shift = 4 * min(distance, count - distance) > count
    ahead = int(length * (AHEAD_LONG if long_shift else AHEAD_SHORT)) // 128 * 128
    pairs = [(i, (i + distance) % count) for i in range(count)]

    current = jnp.concatenate([stay, moved], axis=0)
    raw_in = lax.ppermute(current[:, :ahead], "blk", pairs)
    partial_gram = matmul(current, current, ((1,), (1,)))
    leaving, staying, step_sums = pair_rotation(code, summed_grams(partial_gram))
    rest = matmul(leaving, current[:, ahead:], ((0,), (0,)))
    rest_in = lax.ppermute(rest, "blk", pairs)
    leaving_in = lax.ppermute(leaving, "blk", pairs)
    stay = matmul(staying, current, ((0,), (0,)))
    front_in = matmul(leaving_in, raw_in, ((0,), (0,)))
    moved = jnp.concatenate([front_in, rest_in], axis=1)
    return lax.optimization_barrier((stay, moved, step_sums[:1]))


def local(columns, plan):
    cycle_size = lax.axis_size("blk")
    width = columns.shape[0] // 2
    branches = [partial(one_step, distance=distance) for distance in range(1, cycle_size)]

    slots = (plan[:, 1] != 1).astype(jnp.int32)
    held = jnp.concatenate([jnp.ones((1,), jnp.int32), slots[:-1]])
    flags = (slots == held).astype(jnp.int32)
    shifts = jnp.maximum(plan[:, 0] >> 1, plan[:, 1] >> 1) - 1
    codes, slots = lax.optimization_barrier((2 * shifts + flags, slots))

    def step_body(step_index, carry):
        stay, moved, sums = carry
        code = lax.dynamic_slice(codes, (step_index,), (1,))
        stay, moved, step_sums = lax.switch(code[0] >> 1, branches, stay, moved, code)
        return stay, moved, lax.dynamic_update_slice(sums, step_sums, (step_index, 0))

    carry = (columns[:width], columns[width:], jnp.zeros((STEPS, 128), jnp.float32))
    stay, moved, sums = lax.fori_loop(0, STEPS, step_body, carry)
    totals = sum_over_blk(sums)
    current = jnp.where(
        slots[STEPS - 1] == 1,
        jnp.concatenate([stay, moved], axis=0),
        jnp.concatenate([moved, stay], axis=0),
    )
    return (current, jnp.sqrt(totals[:, 0]) / jnp.sqrt(totals[:, 1]))


def solution(mesh):
    return jax.shard_map(
        local,
        mesh=mesh,
        in_specs=(P("blk", "rows"), P()),
        out_specs=(P("blk", "rows"), P()),
        check_vma=False,
    )
```
